32 devices in a mesh: tensor: 2 (over x), context: 8 (over z, core), dp: 2 (over y).
Axes of the slice: x: 2, y: 2, z: 4, core: 2. Of those that a mesh axis runs over, the one named last changes fastest.
Arguments:
- query_a: bfloat16 [2048, 1024], P(('dp', 'context'), 'tensor'), parts along dimension 0, may hold values from -5 to 5
- key_a: bfloat16 [2048, 256], P(('dp', 'context'), 'tensor'), parts along dimension 0, may hold values from -5 to 5
- value_a: bfloat16 [2048, 256], P(('dp', 'context'), 'tensor'), parts along dimension 0, may hold values from -12 to 12
- grad_out_a: bfloat16 [2048, 1024], P(('dp', 'context'), 'tensor'), parts along dimension 0, may hold values from -6 to 6
- query_b: bfloat16 [2048, 1024], P(('dp', 'context'), 'tensor'), parts along dimension 0, may hold values from -5 to 5
- key_b: bfloat16 [2048, 256], P(('dp', 'context'), 'tensor'), parts along dimension 0, may hold values from -5 to 5
- value_b: bfloat16 [2048, 256], P(('dp', 'context'), 'tensor'), parts along dimension 0, may hold values from -12 to 12
- slab_owner: int32 [8], replicated, may hold values from 0 to 7, each once
Outputs:
- out_b: bfloat16 [2048, 1024], P(('dp', 'context'), 'tensor'), parts along dimension 0
- grad_query_a: bfloat16 [2048, 1024], P(('dp', 'context'), 'tensor'), parts along dimension 0
- grad_key_a: bfloat16 [2048, 256], P(('dp', 'context'), 'tensor'), parts along dimension 0
- grad_value_a: bfloat16 [2048, 256], P(('dp', 'context'), 'tensor'), parts along dimension 0
The draws below stay inside these ranges and needn't reach their ends.
There are 2 independent parts, one for each index of `dp`. The reference program is written for one: setup_inputs(seed, part) draws one part's arguments, and reference() takes and returns one part's arrays. A program takes and returns all parts, laid end to end along the dimension named above; an argument that names none is the same for every part. Nothing has to cross between parts.
Inputs may be any that keep to these rules, and one draw needn't show every extreme that they name: `slab_owner`: each number appears once.
All inputs are finite; a program needn't handle non-finite values.
Results may differ from the reference program's by a relative error of at most 0.0091.
Values may be sent and summed in bfloat16 or wider, within the bound.
No kernel may reach another device: no remote copies, remote signals or barrier semaphores. Data moves between devices by JAX's collectives and lax.ppermute only.
A program may use at most 64 MiB of HBM per device.

```python
import jax
import jax.numpy as jnp
from jax import lax

HEAD_DIM = 128
HEADS_DEV = 4
TOK_DEV = 128
HEADS = 8
KV_HEADS = 2
TOKENS = 1024
N_CONTEXT = 8


def random_base(key, label, width):
    inner = jax.random.fold_in(key, label)
    return jnp.clip(1.4 * jax.random.normal(inner, (TOKENS, width), jnp.float32), -5.0, 5.0)


def drawn_queries(key, label):
    values = random_base(key, label + 1, HEADS * HEAD_DIM)
    return values.astype(jnp.bfloat16)


def drawn_keys(key, label):
    values = random_base(key, label + 7, KV_HEADS * HEAD_DIM)
    return values.astype(jnp.bfloat16)


def draw_query_a(key, part):
    return drawn_queries(key, 101)


def draw_key_a(key, part):
    return drawn_keys(key, 101)


def draw_query_b(key, part):
    return drawn_queries(key, 202)


def draw_key_b(key, part):
    return drawn_keys(key, 202)


def steps_of(stream_key, dims, cuts, low, top_value):
    level, own = 1.0, jax.random.fold_in(stream_key, 6)
    for position, shards_of in cuts:
        steps = jnp.exp(jax.random.uniform(jax.random.fold_in(own, position), (shards_of,), jnp.float32, low / len(cuts), top_value / len(cuts)))
        level = level * jnp.repeat(steps, dims[position] // shards_of).reshape([-1 if axis == position else 1 for axis in range(len(dims))])
    return level


def bell_draw(own_key, shape, spread, reach, pieces=(), held_as=jnp.bfloat16):
    drawn = jax.random.normal(own_key, shape, jnp.float32) * spread
    if len(pieces) > 0:
        drawn = steps_of(own_key, shape, pieces, -0.22, 0.18) * drawn
    return jnp.clip(drawn, min=-reach, max=reach).astype(held_as)


def setup_inputs(seed: int = 0, part: int = 0) -> dict:
    key_of = jax.random.split(jax.random.key(seed), 9)
    own_keys = jax.random.split(jax.random.fold_in(key_of[8], part), 9)
    query_a = draw_query_a(jax.random.fold_in(jax.random.fold_in(key_of[8], part), 71), part)
    key_a = draw_key_a(jax.random.fold_in(jax.random.fold_in(key_of[8], part), 71), part)
    value_a = bell_draw(own_keys[2], (TOKENS, KV_HEADS * HEAD_DIM), 2.0, 12.0, ((0, 8), (1, 2)))
    grad_out_a = bell_draw(own_keys[3], (TOKENS, HEADS * HEAD_DIM), 1.0, 6.0, ((0, 8), (1, 2)))
    query_b = draw_query_b(jax.random.fold_in(jax.random.fold_in(key_of[8], part), 71), part)
    key_b = draw_key_b(jax.random.fold_in(jax.random.fold_in(key_of[8], part), 71), part)
    value_b = bell_draw(own_keys[6], (TOKENS, KV_HEADS * HEAD_DIM), 2.0, 12.0, ((0, 8), (1, 2)))
    slab_owner = jax.random.permutation(key_of[7], N_CONTEXT).astype(jnp.int32)
    return {"query_a": query_a, "key_a": key_a, "value_a": value_a, "grad_out_a": grad_out_a, "query_b": query_b, "key_b": key_b, "value_b": value_b, "slab_owner": slab_owner}


def slab_places(slab_owner):
    half = TOK_DEV // 2
    rows = jnp.arange(TOKENS, dtype=jnp.int32)
    holder = rows // TOK_DEV
    within = rows % TOK_DEV
    owner_slab = slab_owner[holder].astype(jnp.int32)
    slab = jnp.where(within < half, owner_slab, 2 * N_CONTEXT - 1 - owner_slab)
    return (slab * half + within % half).astype(jnp.int32)


def scores_of(queries, keys, query_places, places):
    raw = jnp.einsum("bhd,nd->hbn", queries.astype(jnp.float32), keys.astype(jnp.float32))
    allowed = places[None, None, :] <= query_places[None, :, None]
    return raw * HEAD_DIM ** -0.5, allowed


def forward_rows(queries, query_places, keys, values, places):
    scaled, allowed = scores_of(queries, keys, query_places, places)
    top = jnp.max(jnp.where(allowed, scaled, -jnp.inf), axis=2)
    raised = jnp.where(allowed, jnp.exp(scaled - top[:, :, None]), 0.0)
    total = jnp.sum(raised, axis=2)
    weights = lax.optimization_barrier(raised.astype(jnp.bfloat16))
    summed = jnp.einsum("hbn,nd->bhd", weights.astype(jnp.float32), values.astype(jnp.float32))
    mixed = summed / jnp.transpose(total)[:, :, None]
    return mixed, jnp.transpose(top + jnp.log(total))


def forward_all(queries, keys, values, places):
    query_rows = min(512, TOKENS)
    blocks = TOKENS // query_rows

    def one_block(item):
        return forward_rows(item[0], item[1], keys, values, places)

    mixed, log_total = lax.map(one_block, (queries.reshape(blocks, query_rows, HEADS_DEV, HEAD_DIM), places.reshape(blocks, query_rows)))
    return mixed.reshape(TOKENS, HEADS_DEV, HEAD_DIM), log_total.reshape(TOKENS, HEADS_DEV)


def backward_all(queries, keys, values, grads, places):
    mixed, log_total = forward_all(queries, keys, values, places)
    delta = jnp.sum(grads.astype(jnp.float32) * mixed, axis=2)
    query_rows = min(512, TOKENS)
    blocks = TOKENS // query_rows
    scale = HEAD_DIM ** -0.5

    def advance(carried, item):
        block_query, block_grad, block_places, block_log, block_delta = item
        scaled, allowed = scores_of(block_query, keys, block_places, places)
        prob = jnp.where(allowed, jnp.exp(scaled - jnp.transpose(block_log)[:, :, None]), 0.0)
        prob_grad = jnp.einsum("bhd,nd->hbn", block_grad.astype(jnp.float32), values.astype(jnp.float32))
        score_grad = (prob * (prob_grad - jnp.transpose(block_delta)[:, :, None])).astype(jnp.bfloat16)
        low_prob = prob.astype(jnp.bfloat16)
        score_grad, low_prob = lax.optimization_barrier((score_grad, low_prob))
        query_grad = jnp.einsum("hbn,nd->bhd", score_grad.astype(jnp.float32), keys.astype(jnp.float32)) * scale
        key_sum = carried[0] + jnp.einsum("hbn,bhd->nd", score_grad.astype(jnp.float32), block_query.astype(jnp.float32))
        value_sum = carried[1] + jnp.einsum("hbn,bhd->nd", low_prob.astype(jnp.float32), block_grad.astype(jnp.float32))
        return (key_sum, value_sum), query_grad.astype(jnp.bfloat16)

    items = (queries.reshape(blocks, query_rows, HEADS_DEV, HEAD_DIM), grads.reshape(blocks, query_rows, HEADS_DEV, HEAD_DIM), places.reshape(blocks, query_rows), log_total.reshape(blocks, query_rows, HEADS_DEV), delta.reshape(blocks, query_rows, HEADS_DEV))
    empty = jnp.zeros((TOKENS, HEAD_DIM), jnp.float32)
    sums, query_grad = lax.scan(advance, (empty, empty), items)
    key_grad = (sums[0] * scale).astype(jnp.bfloat16)
    value_grad = sums[1].astype(jnp.bfloat16)
    return query_grad.reshape(TOKENS, HEADS_DEV * HEAD_DIM), key_grad, value_grad


def reference(query_a, key_a, value_a, grad_out_a, query_b, key_b, value_b, slab_owner):
    places = slab_places(slab_owner)
    width = HEADS_DEV * HEAD_DIM
    outs_b = []
    grads_query = []
    grads_key = []
    grads_value = []
    for group in range(KV_HEADS):
        head_lo = group * width
        kv_lo = group * HEAD_DIM
        group_query_b = query_b[:, head_lo:head_lo + width].reshape(TOKENS, HEADS_DEV, HEAD_DIM)
        mixed_b, unused = forward_all(group_query_b, key_b[:, kv_lo:kv_lo + HEAD_DIM], value_b[:, kv_lo:kv_lo + HEAD_DIM], places)
        outs_b.append(mixed_b.reshape(TOKENS, width).astype(jnp.bfloat16))
        group_query_a = query_a[:, head_lo:head_lo + width].reshape(TOKENS, HEADS_DEV, HEAD_DIM)
        group_grad = grad_out_a[:, head_lo:head_lo + width].reshape(TOKENS, HEADS_DEV, HEAD_DIM)
        query_grad, key_grad, value_grad = backward_all(group_query_a, key_a[:, kv_lo:kv_lo + HEAD_DIM], value_a[:, kv_lo:kv_lo + HEAD_DIM], group_grad, places)
        grads_query.append(query_grad)
        grads_key.append(key_grad)
        grads_value.append(value_grad)
    return (jnp.concatenate(outs_b, axis=1), jnp.concatenate(grads_query, axis=1), jnp.concatenate(grads_key, axis=1), jnp.concatenate(grads_value, axis=1))
```

```python
from functools import partial
import math

import jax
import jax.numpy as jnp
from jax import lax
from jax.experimental import pallas as pl
from jax.experimental.pallas import tpu as pltpu
from jax.sharding import PartitionSpec as P


LOW = -1e30
FLOOR = -1e20
F32 = jnp.float32
BF16 = jnp.bfloat16
LOG2E = math.log2(math.e)
VMEM_GRANT = 24 << 20


def dot(a, b, dims):
    return lax.dot_general(a, b, (dims, ((), ())), preferred_element_type=F32)


class Shape:
    def __init__(self, tok, width, dim, devices):
        self.tok, self.width, self.dim, self.devices = tok, width, dim, devices
        self.half = tok // 2
        self.heads = width // dim
        self.chunks = devices // 2
        self.group = self.heads * self.half
        self.keys = self.chunks * self.half
        self.scale = dim ** (-0.5)
        self.exp_scale = self.scale * LOG2E


def offsets(s, owner_ref):
    me = lax.axis_index("context")
    rows = [owner_ref[me], owner_ref[me ^ 1]]
    keys = [owner_ref[me ^ (2 * k)] for k in range(s.chunks)]
    return rows, keys


def stacked(s, own_ref, other_ref):
    parts = []
    for h in range(2):
        for ref in (own_ref, other_ref):
            for g in range(s.heads):
                parts.append(ref[h * s.half:(h + 1) * s.half, g * s.dim:(g + 1) * s.dim])
    return jnp.concatenate(parts, axis=0)


def halves(s, chunk_refs, part):
    cols = slice(part * s.dim, (part + 1) * s.dim)
    low = jnp.concatenate([r[:s.half, cols] for r in chunk_refs], axis=0)
    high = jnp.concatenate([r[s.half:, cols] for r in chunk_refs], axis=0)
    return low, high


def relative(s):
    key = lax.broadcasted_iota(jnp.int32, (s.half, s.group), 0)
    row = lax.broadcasted_iota(jnp.int32, (s.half, s.group), 1) % s.half
    return key - row


def masked(s, scores, rel, row_slab, key_slabs, high):
    parts = []
    for k in range(s.chunks):
        gap = (key_slabs[k] - row_slab) if high else (row_slab - key_slabs[k])
        block = scores[k * s.half:(k + 1) * s.half, :]
        parts.append(jnp.where(rel <= gap * s.half, block, LOW))
    return jnp.concatenate(parts, axis=0)


def stats_kernel(s, owner_ref, qo_ref, qp_ref, go_ref, gp_ref, *refs):
    chunks, out_ref = refs[:-1], refs[-1]
    row_slabs, key_slabs = offsets(s, owner_ref)
    q, g = stacked(s, qo_ref, qp_ref), stacked(s, go_ref, gp_ref)
    k_low, k_high = halves(s, chunks, 0)
    v_low, v_high = halves(s, chunks, 1)
    rel = relative(s)
    for h in range(2):
        for d in range(2):
            at = (2 * h + d) * s.group
            qt, gt = q[at:at + s.group], g[at:at + s.group]
            raw = dot(k_low, qt, ((1,), (1,)))
            pg = dot(v_low, gt, ((1,), (1,)))
            if h == 0:
                raw = masked(s, raw, rel, row_slabs[d], key_slabs, False)
                blocks = [(raw, pg)]
            else:
                more = masked(s, dot(k_high, qt, ((1,), (1,))), rel, row_slabs[d], key_slabs, True)
                blocks = [(raw, pg), (more, dot(v_high, gt, ((1,), (1,))))]
            top = jnp.full((1, s.group), FLOOR, F32)
            for raw, pg in blocks:
                top = jnp.maximum(top, jnp.max(raw, axis=0, keepdims=True))
            total = jnp.zeros((1, s.group), F32)
            dsum = jnp.zeros((1, s.group), F32)
            for raw, pg in blocks:
                p = jnp.exp2((raw - top) * s.exp_scale)
                total = total + jnp.sum(p, axis=0, keepdims=True)
                dsum = dsum + jnp.sum(p * pg, axis=0, keepdims=True)
            out_ref[0:1, at:at + s.group] = top
            out_ref[1:2, at:at + s.group] = total
            out_ref[2:3, at:at + s.group] = dsum
    out_ref[3:8, :] = jnp.zeros((5, 4 * s.group), F32)


def back_kernel(s, owner_ref, qo_ref, qp_ref, go_ref, gp_ref, mine_ref, theirs_ref, *refs):
    chunks = refs[:s.chunks]
    outs = refs[s.chunks:2 * s.chunks]
    dq_own_ref, dq_other_ref, prob_ref, grad_ref = refs[2 * s.chunks:]
    row_slabs, key_slabs = offsets(s, owner_ref)
    q, g = stacked(s, qo_ref, qp_ref), stacked(s, go_ref, gp_ref)
    k_low, k_high = halves(s, chunks, 0)
    v_low, v_high = halves(s, chunks, 1)
    rel = relative(s)
    n, group, keys = 4 * s.group, s.group, s.keys
    for h in range(2):
        for d in range(2):
            at, across = (2 * h + d) * group, (2 * h + 1 - d) * group
            m1, l1, d1 = (mine_ref[i:i + 1, at:at + group] for i in range(3))
            m2, l2, d2 = (theirs_ref[i:i + 1, across:across + group] for i in range(3))
            top = jnp.maximum(m1, m2)
            w1, w2 = jnp.exp2((m1 - top) * s.exp_scale), jnp.exp2((m2 - top) * s.exp_scale)
            total = l1 * w1 + l2 * w2
            delta = (d1 * w1 + d2 * w2) / total
            shift = top * s.exp_scale + jnp.log2(total)
            qt, gt = q[at:at + group], g[at:at + group]
            for b in range(h + 1):
                kk, vv = (k_low, v_low) if b == 0 else (k_high, v_high)
                raw = dot(kk, qt, ((1,), (1,)))
                pg = dot(vv, gt, ((1,), (1,)))
                if b == h:
                    raw = masked(s, raw, rel, row_slabs[d], key_slabs, h == 1)
                p = jnp.exp2(raw * s.exp_scale - shift)
                prob_ref[b * keys:(b + 1) * keys, at:at + group] = p.astype(BF16)
                grad_ref[b * keys:(b + 1) * keys, at:at + group] = (p * (pg - delta)).astype(BF16)
    mid = 2 * group
    dk_low = dot(grad_ref[:keys, :], q, ((1,), (0,))) * s.scale
    dv_low = dot(prob_ref[:keys, :], g, ((1,), (0,)))
    dk_high = dot(grad_ref[keys:, mid:], q[mid:], ((1,), (0,))) * s.scale
    dv_high = dot(prob_ref[keys:, mid:], g[mid:], ((1,), (0,)))
    for k in range(s.chunks):
        at = slice(k * s.half, (k + 1) * s.half)
        kind = outs[k].dtype
        outs[k][:s.half, :s.dim] = dk_low[at].astype(kind)
        outs[k][:s.half, s.dim:] = dv_low[at].astype(kind)
        outs[k][s.half:, :s.dim] = dk_high[at].astype(kind)
        outs[k][s.half:, s.dim:] = dv_high[at].astype(kind)
    low_rows = dot(k_low, grad_ref[:keys, :mid], ((0,), (0,)))
    high_rows = dot(k_low, grad_ref[:keys, mid:], ((0,), (0,)))
    high_rows = high_rows + dot(k_high, grad_ref[keys:, mid:], ((0,), (0,)))
    for d, ref in enumerate((dq_own_ref, dq_other_ref)):
        ref[:, :group] = low_rows[:, d * group:(d + 1) * group]
        ref[:, group:] = high_rows[:, d * group:(d + 1) * group]


def forward_kernel(s, owner_ref, qo_ref, qp_ref, *refs):
    chunks, outs = refs[:-2], refs[-2:]
    row_slabs, key_slabs = offsets(s, owner_ref)
    q = stacked(s, qo_ref, qp_ref)
    k_low, k_high = halves(s, chunks, 0)
    v_low, v_high = halves(s, chunks, 1)
    rel = relative(s)
    for h in range(2):
        for d in range(2):
            at = (2 * h + d) * s.group
            qt = q[at:at + s.group]
            raw = dot(k_low, qt, ((1,), (1,)))
            if h == 0:
                blocks = [(masked(s, raw, rel, row_slabs[d], key_slabs, False), v_low)]
            else:
                more = dot(k_high, qt, ((1,), (1,)))
                more = masked(s, more, rel, row_slabs[d], key_slabs, True)
                blocks = [(raw, v_low), (more, v_high)]
            top = jnp.full((1, s.group), FLOOR, F32)
            for raw, vv in blocks:
                top = jnp.maximum(top, jnp.max(raw, axis=0, keepdims=True))
            total = jnp.zeros((1, s.group), F32)
            acc = jnp.zeros((s.dim, s.group), F32)
            for raw, vv in blocks:
                p = jnp.exp2((raw - top) * s.exp_scale)
                total = total + jnp.sum(p, axis=0, keepdims=True)
                acc = acc + dot(vv, p.astype(BF16), ((0,), (0,)))
            cols = slice(h * s.group, (h + 1) * s.group)
            outs[d][:s.dim, cols] = acc
            outs[d][s.dim:s.dim + 1, cols] = top
            outs[d][s.dim + 1:s.dim + 2, cols] = total
            outs[d][s.dim + 2:s.dim + 8, cols] = jnp.zeros((6, s.group), F32)


def rows_from(s, wide, out_ref):
    for h in range(2):
        for g in range(s.heads):
            at = h * s.group + g * s.half
            block = wide[:, at:at + s.half]
            out_ref[h * s.half:(h + 1) * s.half, g * s.dim:(g + 1) * s.dim] = block.T.astype(BF16)


def query_kernel(s, own_ref, other_ref, out_ref):
    rows_from(s, (own_ref[...] + other_ref[...]) * s.scale, out_ref)


def merge_kernel(s, own_ref, other_ref, out_ref):
    d = s.dim
    m1, l1 = own_ref[d:d + 1, :], own_ref[d + 1:d + 2, :]
    m2, l2 = other_ref[d:d + 1, :], other_ref[d + 1:d + 2, :]
    top = jnp.maximum(m1, m2)
    w1, w2 = jnp.exp2((m1 - top) * s.exp_scale), jnp.exp2((m2 - top) * s.exp_scale)
    total = l1 * w1 + l2 * w2
    rows_from(s, own_ref[:d, :] * (w1 / total) + other_ref[:d, :] * (w2 / total), out_ref)


def sum_kernel(s, *refs):
    terms, (key_ref, value_ref) = refs[:-2], refs[-2:]
    acc = terms[0][...]
    for t in terms[1:]:
        acc = acc + t[...].astype(F32)
    key_ref[...] = acc[:, :s.dim].astype(BF16)
    value_ref[...] = acc[:, s.dim:].astype(BF16)


def call(kernel, name, outs, args, flops, owner=True, scratch=()):
    specs = [pl.BlockSpec(memory_space=pltpu.VMEM)] * len(args)
    if owner:
        specs[0] = pl.BlockSpec(memory_space=pltpu.SMEM)
    return pl.pallas_call(
        kernel,
        name=name,
        out_shape=outs,
        in_specs=specs,
        out_specs=jax.tree.map(lambda _: pl.BlockSpec(memory_space=pltpu.VMEM), outs),
        scratch_shapes=scratch,
        compiler_params=pltpu.CompilerParams(vmem_limit_bytes=VMEM_GRANT),
        cost_estimate=pl.CostEstimate(flops=flops, bytes_accessed=1 << 20, transcendentals=0),
    )(*args)


def on_device(query_a, key_a, value_a, grad_out_a, query_b, key_b, value_b, slab_owner):
    devices = lax.axis_size("context")
    tok, width = query_a.shape
    s = Shape(tok, width, key_a.shape[1], devices)
    dim, group = s.dim, s.group

    def swapped(x, bits):
        return lax.ppermute(x, "context", [(i, i ^ bits) for i in range(devices)])

    def sds(shape, dtype):
        return jax.ShapeDtypeStruct(shape, dtype)

    def gathered(x):
        return [x] + [swapped(x, 2 * k) for k in range(1, s.chunks)]

    kv_a = gathered(jnp.concatenate([key_a, value_a], axis=1))
    query_p, grad_p = swapped(query_a, 1), swapped(grad_out_a, 1)
    kv_b = gathered(jnp.concatenate([key_b, value_b], axis=1))
    query_bp = swapped(query_b, 1)

    unit = 2 * 4 * group * s.keys * dim
    mine = call(
        partial(stats_kernel, s), "stats", sds((8, 4 * group), F32),
        [slab_owner, query_a, query_p, grad_out_a, grad_p, *kv_a], 8 * unit,
    )
    theirs = swapped(mine, 1)
    kinds = [F32] + [BF16] * (s.chunks - 1)
    back = call(
        partial(back_kernel, s), "back",
        [sds((tok, 2 * dim), kind) for kind in kinds] + [sds((dim, 2 * group), F32)] * 2,
        [slab_owner, query_a, query_p, grad_out_a, grad_p, mine, theirs, *kv_a], 20 * unit,
        scratch=[pltpu.VMEM((2 * s.keys, 4 * group), BF16)] * 2,
    )
    terms, (dq_own, dq_other) = back[:s.chunks], back[s.chunks:]
    terms = [terms[0]] + [swapped(terms[k], 2 * k) for k in range(1, s.chunks)]
    dq_got = swapped(dq_other, 1)

    part_own, part_other = call(
        partial(forward_kernel, s), "forward", [sds((dim + 8, 2 * group), F32)] * 2,
        [slab_owner, query_b, query_bp, *kv_b], 10 * unit,
    )
    part_got = swapped(part_other, 1)
    grad_query_a = call(
        partial(query_kernel, s), "query", sds((tok, width), BF16), [dq_own, dq_got], unit, owner=False
    )
    out_b = call(
        partial(merge_kernel, s), "merge", sds((tok, width), BF16), [part_own, part_got], unit, owner=False
    )
    grad_key_a, grad_value_a = call(
        partial(sum_kernel, s), "total", [sds((tok, dim), BF16)] * 2, terms, unit, owner=False
    )
    return (out_b, grad_query_a, grad_key_a, grad_value_a)


def solution(mesh):
    rows = P(("dp", "context"), "tensor")
    return jax.shard_map(
        on_device,
        mesh=mesh,
        in_specs=(rows,) * 7 + (P(),),
        out_specs=(rows,) * 4,
        check_vma=False,
    )
```

```python
from functools import partial
import math

import jax
import jax.numpy as jnp
from jax import lax
from jax.experimental import pallas as pl
from jax.experimental.pallas import tpu as pltpu
from jax.sharding import PartitionSpec as P


LOW = -1e30
FLOOR = -1e20
F32 = jnp.float32
BF16 = jnp.bfloat16
LOG2E = math.log2(math.e)
VMEM_GRANT = 24 << 20


def dot(a, b, dims):
    return lax.dot_general(a, b, (dims, ((), ())), preferred_element_type=F32)


class Shape:
    def __init__(self, tok, width, dim, devices):
        self.tok, self.width, self.dim, self.devices = tok, width, dim, devices
        self.half = tok // 2
        self.heads = width // dim
        self.chunks = devices // 2
        self.group = self.heads * self.half
        self.keys = self.chunks * self.half
        self.scale = dim ** (-0.5)
        self.exp_scale = self.scale * LOG2E


def stacked(s, own_ref, other_ref):
    parts = []
    for h in range(2):
        for ref in (own_ref, other_ref):
            for g in range(s.heads):
                parts.append(ref[h * s.half:(h + 1) * s.half, g * s.dim:(g + 1) * s.dim])
    return jnp.concatenate(parts, axis=0)


def halves(s, chunk_refs, part):
    cols = slice(part * s.dim, (part + 1) * s.dim)
    low = jnp.concatenate([r[:s.half, cols] for r in chunk_refs], axis=0)
    high = jnp.concatenate([r[s.half:, cols] for r in chunk_refs], axis=0)
    return low, high


def relative(s):
    key = lax.broadcasted_iota(jnp.int32, (s.half, s.group), 0)
    row = lax.broadcasted_iota(jnp.int32, (s.half, s.group), 1) % s.half
    return key - row


def masked(s, scores, rel, gap_ref, d, high):
    parts = []
    for k in range(s.chunks):
        gap = gap_ref[d * s.chunks + k:d * s.chunks + k + 1, :]
        block = scores[k * s.half:(k + 1) * s.half, :]
        parts.append(jnp.where(rel <= (-gap if high else gap), block, LOW))
    return jnp.concatenate(parts, axis=0)


def fetch_kernel(s, owner, ka, va, qa, ga, kb, vb, qb, kv_a, kv_b, query_a, grad_a, query_b, gap, slabs, sems):
    cols = [pl.ds(i * s.dim, s.dim) for i in range(2)]
    moves = [
        (owner, slabs), (ka, kv_a.at[:, cols[0]]), (va, kv_a.at[:, cols[1]]),
        (kb, kv_b.at[:, cols[0]]), (vb, kv_b.at[:, cols[1]]),
        (qa, query_a), (ga, grad_a), (qb, query_b),
    ]
    copies = [pltpu.make_async_copy(a, b, sems.at[i]) for i, (a, b) in enumerate(moves)]
    for c in copies:
        c.start()
    copies[0].wait()
    me = lax.axis_index("context")
    for d in range(2):
        for k in range(s.chunks):
            ahead = (slabs[me ^ d] - slabs[me ^ (2 * k)]) * s.half
            gap[d * s.chunks + k:d * s.chunks + k + 1, :] = jnp.full((1, s.group), ahead, jnp.int32)
    for c in copies[1:]:
        c.wait()


def stack_kernel(s, *refs):
    count = len(refs) // 3
    for i in range(count):
        refs[2 * count + i][...] = stacked(s, refs[2 * i], refs[2 * i + 1])


def pack_kernel(*refs):
    at = 0
    for ref in refs[:-1]:
        refs[-1][at:at + ref.shape[0]] = ref[...]
        at += ref.shape[0]


def stats_kernel(s, gap_ref, q_ref, g_ref, *refs):
    chunks, out_ref = refs[:-1], refs[-1]
    q, g = q_ref[...], g_ref[...]
    k_low, k_high = halves(s, chunks, 0)
    v_low, v_high = halves(s, chunks, 1)
    rel = relative(s)
    for h in range(2):
        for d in range(2):
            at = (2 * h + d) * s.group
            qt, gt = q[at:at + s.group], g[at:at + s.group]
            raw = dot(k_low, qt, ((1,), (1,)))
            pg = dot(v_low, gt, ((1,), (1,)))
            if h == 0:
                raw = masked(s, raw, rel, gap_ref, d, False)
                blocks = [(raw, pg)]
            else:
                more = masked(s, dot(k_high, qt, ((1,), (1,))), rel, gap_ref, d, True)
                blocks = [(raw, pg), (more, dot(v_high, gt, ((1,), (1,))))]
            top = jnp.full((1, s.group), FLOOR, F32)
            for raw, pg in blocks:
                top = jnp.maximum(top, jnp.max(raw, axis=0, keepdims=True))
            total = jnp.zeros((1, s.group), F32)
            dsum = jnp.zeros((1, s.group), F32)
            for raw, pg in blocks:
                p = jnp.exp2((raw - top) * s.exp_scale)
                total = total + jnp.sum(p, axis=0, keepdims=True)
                dsum = dsum + jnp.sum(p * pg, axis=0, keepdims=True)
            out_ref[0:1, at:at + s.group] = top
            out_ref[1:2, at:at + s.group] = total
            out_ref[2:3, at:at + s.group] = dsum
    out_ref[3:8, :] = jnp.zeros((5, 4 * s.group), F32)


def back_kernel(s, gap_ref, q_ref, g_ref, mine_ref, theirs_ref, *refs):
    chunks = refs[:s.chunks]
    outs = refs[s.chunks:2 * s.chunks]
    dq_own_ref, dq_other_ref, prob_ref, grad_ref = refs[2 * s.chunks:]
    q, g = q_ref[...], g_ref[...]
    k_low, k_high = halves(s, chunks, 0)
    v_low, v_high = halves(s, chunks, 1)
    rel = relative(s)
    group, keys = s.group, s.keys
    for h in range(2):
        for d in range(2):
            at, across = (2 * h + d) * group, (2 * h + 1 - d) * group
            m1, l1, d1 = (mine_ref[i:i + 1, at:at + group] for i in range(3))
            m2, l2, d2 = (theirs_ref[i:i + 1, across:across + group] for i in range(3))
            top = jnp.maximum(m1, m2)
            w1, w2 = jnp.exp2((m1 - top) * s.exp_scale), jnp.exp2((m2 - top) * s.exp_scale)
            total = l1 * w1 + l2 * w2
            delta = (d1 * w1 + d2 * w2) / total
            shift = top * s.exp_scale + jnp.log2(total)
            qt, gt = q[at:at + group], g[at:at + group]
            for b in range(h + 1):
                kk, vv = (k_low, v_low) if b == 0 else (k_high, v_high)
                raw = dot(kk, qt, ((1,), (1,)))
                pg = dot(vv, gt, ((1,), (1,)))
                if b == h:
                    raw = masked(s, raw, rel, gap_ref, d, h == 1)
                p = jnp.exp2(raw * s.exp_scale - shift)
                prob_ref[b * keys:(b + 1) * keys, at:at + group] = p.astype(BF16)
                grad_ref[b * keys:(b + 1) * keys, at:at + group] = (p * (pg - delta)).astype(BF16)
    mid = 2 * group
    dk_low = dot(grad_ref[:keys, :], q, ((1,), (0,))) * s.scale
    dv_low = dot(prob_ref[:keys, :], g, ((1,), (0,)))
    dk_high = dot(grad_ref[keys:, mid:], q[mid:], ((1,), (0,))) * s.scale
    dv_high = dot(prob_ref[keys:, mid:], g[mid:], ((1,), (0,)))
    for k in range(s.chunks):
        at = slice(k * s.half, (k + 1) * s.half)
        kind = outs[k].dtype
        outs[k][:s.half, :s.dim] = dk_low[at].astype(kind)
        outs[k][:s.half, s.dim:] = dv_low[at].astype(kind)
        outs[k][s.half:, :s.dim] = dk_high[at].astype(kind)
        outs[k][s.half:, s.dim:] = dv_high[at].astype(kind)
    low_rows = dot(k_low, grad_ref[:keys, :mid], ((0,), (0,)))
    high_rows = dot(k_low, grad_ref[:keys, mid:], ((0,), (0,)))
    high_rows = high_rows + dot(k_high, grad_ref[keys:, mid:], ((0,), (0,)))
    for d, ref in enumerate((dq_own_ref, dq_other_ref)):
        ref[:, :group] = low_rows[:, d * group:(d + 1) * group]
        ref[:, group:] = high_rows[:, d * group:(d + 1) * group]


def forward_kernel(s, names, gap_ref, q_ref, *refs):
    chunks, outs = refs[:-2], refs[-2:]
    q = q_ref[...]
    blocks = [r[k * s.tok:(k + 1) * s.tok] for r in chunks for k in range(r.shape[0] // s.tok)]
    blocks = [blocks[names.index(k)] for k in range(s.chunks)]
    k_low, k_high = halves(s, blocks, 0)
    v_low, v_high = halves(s, blocks, 1)
    rel = relative(s)
    for h in range(2):
        for d in range(2):
            at = (2 * h + d) * s.group
            qt = q[at:at + s.group]
            raw = dot(k_low, qt, ((1,), (1,)))
            if h == 0:
                blocks = [(masked(s, raw, rel, gap_ref, d, False), v_low)]
            else:
                more = dot(k_high, qt, ((1,), (1,)))
                more = masked(s, more, rel, gap_ref, d, True)
                blocks = [(raw, v_low), (more, v_high)]
            top = jnp.full((1, s.group), FLOOR, F32)
            for raw, vv in blocks:
                top = jnp.maximum(top, jnp.max(raw, axis=0, keepdims=True))
            total = jnp.zeros((1, s.group), F32)
            acc = jnp.zeros((s.dim, s.group), F32)
            for raw, vv in blocks:
                p = jnp.exp2((raw - top) * s.exp_scale)
                total = total + jnp.sum(p, axis=0, keepdims=True)
                acc = acc + dot(vv, p.astype(BF16), ((0,), (0,)))
            cols = slice(h * s.group, (h + 1) * s.group)
            outs[d][:s.dim, cols] = acc
            outs[d][s.dim:s.dim + 1, cols] = top
            outs[d][s.dim + 1:s.dim + 2, cols] = total
            outs[d][s.dim + 2:s.dim + 8, cols] = jnp.zeros((6, s.group), F32)


def rows_from(s, wide, out_ref):
    for h in range(2):
        for g in range(s.heads):
            at = h * s.group + g * s.half
            block = wide[:, at:at + s.half]
            out_ref[h * s.half:(h + 1) * s.half, g * s.dim:(g + 1) * s.dim] = block.T.astype(BF16)


def query_kernel(s, own_ref, other_ref, out_ref):
    rows_from(s, (own_ref[...] + other_ref[...]) * s.scale, out_ref)


def merge_kernel(s, own_ref, other_ref, out_ref):
    d = s.dim
    m1, l1 = own_ref[d:d + 1, :], own_ref[d + 1:d + 2, :]
    m2, l2 = other_ref[d:d + 1, :], other_ref[d + 1:d + 2, :]
    top = jnp.maximum(m1, m2)
    w1, w2 = jnp.exp2((m1 - top) * s.exp_scale), jnp.exp2((m2 - top) * s.exp_scale)
    total = l1 * w1 + l2 * w2
    rows_from(s, own_ref[:d, :] * (w1 / total) + other_ref[:d, :] * (w2 / total), out_ref)


def sum_kernel(s, *refs):
    terms, (key_ref, value_ref) = refs[:-2], refs[-2:]
    acc = terms[0][...]
    for t in terms[1:]:
        acc = acc + t[...].astype(F32)
    key_ref[...] = acc[:, :s.dim].astype(BF16)
    value_ref[...] = acc[:, s.dim:].astype(BF16)


def call(kernel, outs, args, flops, scratch=(), space=pltpu.VMEM):
    specs = [pl.BlockSpec(memory_space=space)] * len(args)
    if space == pltpu.HBM:
        args = [pltpu.with_memory_space_constraint(a, space) for a in args]
    return pl.pallas_call(
        kernel,
        out_shape=outs,
        in_specs=specs,
        out_specs=jax.tree.map(lambda _: pl.BlockSpec(memory_space=pltpu.VMEM), outs),
        scratch_shapes=scratch,
        compiler_params=pltpu.CompilerParams(vmem_limit_bytes=VMEM_GRANT),
        cost_estimate=pl.CostEstimate(flops=flops, bytes_accessed=1 << 20, transcendentals=0),
    )(*args)


def on_device(query_a, key_a, value_a, grad_out_a, query_b, key_b, value_b, slab_owner):
    devices = lax.axis_size("context")
    tok, width = query_a.shape
    s = Shape(tok, width, key_a.shape[1], devices)
    dim, group = s.dim, s.group

    def swapped(x, bits):
        return lax.ppermute(x, "context", [(i, i ^ bits) for i in range(devices)])

    def sds(shape, dtype):
        return jax.ShapeDtypeStruct(shape, dtype)

    unit = 2 * 4 * group * s.keys * dim
    wide, pair, stack = sds((tok, width), BF16), sds((tok, 2 * dim), BF16), sds((4 * group, dim), BF16)
    kv_a, kv_b, query_a, grad_a, query_b, gap = call(
        partial(fetch_kernel, s), [pair, pair, wide, wide, wide, sds((2 * s.chunks, group), jnp.int32)],
        [slab_owner, key_a, value_a, query_a, grad_out_a, key_b, value_b, query_b], unit,
        space=pltpu.HBM, scratch=[pltpu.SMEM((devices,), jnp.int32), pltpu.SemaphoreType.DMA((8,))],
    )
    held, bit = {0: kv_a}, s.chunks // 2
    while bit:
        held.update({k ^ bit: swapped(x, 2 * bit) for k, x in list(held.items())})
        bit //= 2
    kv_a = [held[k] for k in range(s.chunks)]
    query_p, grad_p = swapped(query_a, 1), swapped(grad_a, 1)
    query_bp = swapped(query_b, 1)
    q_a, g_a = call(partial(stack_kernel, s), [stack, stack], [query_a, query_p, grad_a, grad_p], unit)
    mine = call(partial(stats_kernel, s), sds((8, 4 * group), F32), [gap, q_a, g_a, *kv_a], 8 * unit)
    order_b, bit = [0], s.chunks // 2
    while bit:
        if len(order_b) > 1:
            kv_b = call(pack_kernel, sds((len(order_b) * tok, 2 * dim), BF16), parts, unit)
        parts = [kv_b, swapped(kv_b, 2 * bit)]
        order_b += [k ^ bit for k in order_b]
        bit //= 2
    kv_b = parts
    theirs = swapped(mine, 1)
    kinds = [F32] + [BF16] * (s.chunks - 1)
    back = call(
        partial(back_kernel, s),
        [sds((tok, 2 * dim), kind) for kind in kinds] + [sds((dim, 2 * group), F32)] * 2,
        [gap, q_a, g_a, mine, theirs, *kv_a], 20 * unit,
        scratch=[pltpu.VMEM((2 * s.keys, 4 * group), BF16)] * 2,
    )
    terms, (dq_own, dq_other) = back[:s.chunks], back[s.chunks:]
    terms = [terms[0]] + [swapped(terms[k], 2 * k) for k in range(1, s.chunks)]
    dq_got = swapped(dq_other, 1)

    (q_b,) = call(partial(stack_kernel, s), [stack], [query_b, query_bp], unit)
    part_own, part_other = call(
        partial(forward_kernel, s, order_b), [sds((dim + 8, 2 * group), F32)] * 2,
        [gap, q_b, *kv_b], 10 * unit,
    )
    part_got = swapped(part_other, 1)
    grad_query_a = call(partial(query_kernel, s), sds((tok, width), BF16), [dq_own, dq_got], unit)
    out_b = call(partial(merge_kernel, s), sds((tok, width), BF16), [part_own, part_got], unit)
    grad_key_a, grad_value_a = call(partial(sum_kernel, s), [sds((tok, dim), BF16)] * 2, terms, unit)
    return (out_b, grad_query_a, grad_key_a, grad_value_a)


def solution(mesh):
    rows = P(("dp", "context"), "tensor")

    return jax.shard_map(
        on_device,
        mesh=mesh,
        in_specs=(rows,) * 7 + (P(),),
        out_specs=(rows,) * 4,
        check_vma=False,
    )
```

```python
from functools import partial
import math

import jax
import jax.numpy as jnp
from jax import lax
from jax.experimental import pallas as pl
from jax.experimental.pallas import tpu as pltpu
from jax.sharding import PartitionSpec as P


LOW = -1e30
FLOOR = -1e20
F32 = jnp.float32
BF16 = jnp.bfloat16
LOG2E = math.log2(math.e)
VMEM_GRANT = 24 << 20


def dot(a, b, dims):
    return lax.dot_general(a, b, (dims, ((), ())), preferred_element_type=F32)


class Shape:
    def __init__(self, tok, width, dim, devices):
        self.tok, self.width, self.dim, self.devices = tok, width, dim, devices
        self.half = tok // 2
        self.heads = width // dim
        self.chunks = devices // 2
        self.group = self.heads * self.half
        self.keys = self.chunks * self.half
        self.scale = dim ** (-0.5)
        self.exp_scale = self.scale * LOG2E


def stacked(s, own_ref, other_ref):
    parts = []
    for h in range(2):
        for ref in (own_ref, other_ref):
            for g in range(s.heads):
                parts.append(ref[h * s.half:(h + 1) * s.half, g * s.dim:(g + 1) * s.dim])
    return jnp.concatenate(parts, axis=0)


def halves(s, chunk_refs, part):
    cols = slice(part * s.dim, (part + 1) * s.dim)
    low = jnp.concatenate([r[:s.half, cols] for r in chunk_refs], axis=0)
    high = jnp.concatenate([r[s.half:, cols] for r in chunk_refs], axis=0)
    return low, high


def relative(s):
    key = lax.broadcasted_iota(jnp.int32, (s.half, s.group), 0)
    row = lax.broadcasted_iota(jnp.int32, (s.half, s.group), 1) % s.half
    return key - row


def masked(s, scores, rel, gap_ref, d, high):
    parts = []
    for k in range(s.chunks):
        gap = gap_ref[d * s.chunks + k:d * s.chunks + k + 1, :]
        block = scores[k * s.half:(k + 1) * s.half, :]
        parts.append(jnp.where(rel <= (-gap if high else gap), block, LOW))
    return jnp.concatenate(parts, axis=0)


def fetch_kernel(s, keys, values, out, sems):
    left = pltpu.make_async_copy(keys, out.at[:, pl.ds(0, s.dim)], sems.at[0])
    right = pltpu.make_async_copy(values, out.at[:, pl.ds(s.dim, s.dim)], sems.at[1])
    left.start()
    right.start()
    left.wait()
    right.wait()


def fetch_rest_kernel(s, owner, kb, vb, qa, ga, qb, kv_b, rows, gap, slabs, sems):
    moves = [(owner, slabs), (kb, kv_b.at[:, pl.ds(0, s.dim)]), (vb, kv_b.at[:, pl.ds(s.dim, s.dim)])]
    moves += [(x, rows.at[:, pl.ds(i * s.width, s.width)]) for i, x in enumerate((qa, ga, qb))]
    copies = [pltpu.make_async_copy(a, b, sems.at[i]) for i, (a, b) in enumerate(moves)]
    for c in copies:
        c.start()
    copies[0].wait()
    me = lax.axis_index("context")
    for d in range(2):
        for k in range(s.chunks):
            ahead = (slabs[me ^ d] - slabs[me ^ (2 * k)]) * s.half
            gap[d * s.chunks + k:d * s.chunks + k + 1, :] = jnp.full((1, s.group), ahead, jnp.int32)
    for c in copies[1:]:
        c.wait()


def stack_kernel(s, own_ref, other_ref, *out_refs):
    for i, ref in enumerate(out_refs):
        cols = slice(i * s.width, (i + 1) * s.width)
        ref[...] = stacked(s, own_ref[:, cols], other_ref[:, cols])


def stats_kernel(s, gap_ref, q_ref, g_ref, *refs):
    chunks, out_ref = refs[:-1], refs[-1]
    q, g = q_ref[...], g_ref[...]
    k_low, k_high = halves(s, chunks, 0)
    v_low, v_high = halves(s, chunks, 1)
    rel = relative(s)
    for h in range(2):
        for d in range(2):
            at = (2 * h + d) * s.group
            qt, gt = q[at:at + s.group], g[at:at + s.group]
            raw = dot(k_low, qt, ((1,), (1,)))
            pg = dot(v_low, gt, ((1,), (1,)))
            if h == 0:
                raw = masked(s, raw, rel, gap_ref, d, False)
                blocks = [(raw, pg)]
            else:
                more = masked(s, dot(k_high, qt, ((1,), (1,))), rel, gap_ref, d, True)
                blocks = [(raw, pg), (more, dot(v_high, gt, ((1,), (1,))))]
            top = jnp.full((1, s.group), FLOOR, F32)
            for raw, pg in blocks:
                top = jnp.maximum(top, jnp.max(raw, axis=0, keepdims=True))
            total = jnp.zeros((1, s.group), F32)
            dsum = jnp.zeros((1, s.group), F32)
            for raw, pg in blocks:
                p = jnp.exp2((raw - top) * s.exp_scale)
                total = total + jnp.sum(p, axis=0, keepdims=True)
                dsum = dsum + jnp.sum(p * pg, axis=0, keepdims=True)
            out_ref[0:1, at:at + s.group] = top
            out_ref[1:2, at:at + s.group] = total
            out_ref[2:3, at:at + s.group] = dsum
    out_ref[3:8, :] = jnp.zeros((5, 4 * s.group), F32)


def back_kernel(s, gap_ref, q_ref, g_ref, mine_ref, theirs_ref, *refs):
    chunks = refs[:s.chunks]
    outs = refs[s.chunks:2 * s.chunks]
    dq_own_ref, dq_other_ref, prob_ref, grad_ref = refs[2 * s.chunks:]
    q, g = q_ref[...], g_ref[...]
    k_low, k_high = halves(s, chunks, 0)
    v_low, v_high = halves(s, chunks, 1)
    rel = relative(s)
    group, keys = s.group, s.keys
    for h in range(2):
        for d in range(2):
            at, across = (2 * h + d) * group, (2 * h + 1 - d) * group
            m1, l1, d1 = (mine_ref[i:i + 1, at:at + group] for i in range(3))
            m2, l2, d2 = (theirs_ref[i:i + 1, across:across + group] for i in range(3))
            top = jnp.maximum(m1, m2)
            w1, w2 = jnp.exp2((m1 - top) * s.exp_scale), jnp.exp2((m2 - top) * s.exp_scale)
            total = l1 * w1 + l2 * w2
            delta = (d1 * w1 + d2 * w2) / total
            shift = top * s.exp_scale + jnp.log2(total)
            qt, gt = q[at:at + group], g[at:at + group]
            for b in range(h + 1):
                kk, vv = (k_low, v_low) if b == 0 else (k_high, v_high)
                raw = dot(kk, qt, ((1,), (1,)))
                pg = dot(vv, gt, ((1,), (1,)))
                if b == h:
                    raw = masked(s, raw, rel, gap_ref, d, h == 1)
                p = jnp.exp2(raw * s.exp_scale - shift)
                prob_ref[b * keys:(b + 1) * keys, at:at + group] = p.astype(BF16)
                grad_ref[b * keys:(b + 1) * keys, at:at + group] = (p * (pg - delta)).astype(BF16)
    mid = 2 * group
    dk_low = dot(grad_ref[:keys, :], q, ((1,), (0,))) * s.scale
    dv_low = dot(prob_ref[:keys, :], g, ((1,), (0,)))
    dk_high = dot(grad_ref[keys:, mid:], q[mid:], ((1,), (0,))) * s.scale
    dv_high = dot(prob_ref[keys:, mid:], g[mid:], ((1,), (0,)))
    for k in range(s.chunks):
        at = slice(k * s.half, (k + 1) * s.half)
        kind = outs[k].dtype
        outs[k][:s.half, :s.dim] = dk_low[at].astype(kind)
        outs[k][:s.half, s.dim:] = dv_low[at].astype(kind)
        outs[k][s.half:, :s.dim] = dk_high[at].astype(kind)
        outs[k][s.half:, s.dim:] = dv_high[at].astype(kind)
    low_rows = dot(k_low, grad_ref[:keys, :mid], ((0,), (0,)))
    high_rows = dot(k_low, grad_ref[:keys, mid:], ((0,), (0,)))
    high_rows = high_rows + dot(k_high, grad_ref[keys:, mid:], ((0,), (0,)))
    for d, ref in enumerate((dq_own_ref, dq_other_ref)):
        ref[:, :group] = low_rows[:, d * group:(d + 1) * group]
        ref[:, group:] = high_rows[:, d * group:(d + 1) * group]


def forward_rows(s, d, gap_ref, q_ref, chunks, out_ref):
    k_low, k_high = halves(s, chunks, 0)
    v_low, v_high = halves(s, chunks, 1)
    rel = relative(s)
    for h in range(2):
        at = (2 * h + d) * s.group
        qt = q_ref[at:at + s.group]
        raw = dot(k_low, qt, ((1,), (1,)))
        if h == 0:
            blocks = [(masked(s, raw, rel, gap_ref, d, False), v_low)]
        else:
            more = dot(k_high, qt, ((1,), (1,)))
            blocks = [(raw, v_low), (masked(s, more, rel, gap_ref, d, True), v_high)]
        top = jnp.full((1, s.group), FLOOR, F32)
        for raw, vv in blocks:
            top = jnp.maximum(top, jnp.max(raw, axis=0, keepdims=True))
        total = jnp.zeros((1, s.group), F32)
        acc = jnp.zeros((s.dim, s.group), F32)
        for raw, vv in blocks:
            p = jnp.exp2((raw - top) * s.exp_scale)
            total = total + jnp.sum(p, axis=0, keepdims=True)
            acc = acc + dot(vv, p.astype(BF16), ((0,), (0,)))
        cols = slice(h * s.group, (h + 1) * s.group)
        out_ref[:s.dim, cols] = acc
        out_ref[s.dim:s.dim + 1, cols] = top
        out_ref[s.dim + 1:s.dim + 2, cols] = total
        out_ref[s.dim + 2:s.dim + 8, cols] = jnp.zeros((6, s.group), F32)


def other_kernel(s, gap_ref, q_ref, dq_ref, *refs):
    chunks, out_ref = refs[:-1], refs[-1]
    forward_rows(s, 1, gap_ref, q_ref, chunks, out_ref)
    out_ref[s.dim + 8:, :] = dq_ref[...]


def own_kernel(s, gap_ref, q_ref, after, *refs):
    forward_rows(s, 0, gap_ref, q_ref, refs[:-1], refs[-1])


def rows_from(s, wide, out_ref):
    for h in range(2):
        for g in range(s.heads):
            at = h * s.group + g * s.half
            block = wide[:, at:at + s.half]
            out_ref[h * s.half:(h + 1) * s.half, g * s.dim:(g + 1) * s.dim] = block.T.astype(BF16)


def rows_kernel(s, own_ref, dq_ref, got_ref, out_ref, query_ref):
    d = s.dim
    rows_from(s, (dq_ref[...] + got_ref[d + 8:, :]) * s.scale, query_ref)
    m1, l1 = own_ref[d:d + 1, :], own_ref[d + 1:d + 2, :]
    m2, l2 = got_ref[d:d + 1, :], got_ref[d + 1:d + 2, :]
    top = jnp.maximum(m1, m2)
    w1, w2 = jnp.exp2((m1 - top) * s.exp_scale), jnp.exp2((m2 - top) * s.exp_scale)
    total = l1 * w1 + l2 * w2
    rows_from(s, own_ref[:d, :] * (w1 / total) + got_ref[:d, :] * (w2 / total), out_ref)


def sum_kernel(s, *refs):
    terms, (key_ref, value_ref) = refs[:-2], refs[-2:]
    acc = terms[0][...]
    for t in terms[1:]:
        acc = acc + t[...].astype(F32)
    key_ref[...] = acc[:, :s.dim].astype(BF16)
    value_ref[...] = acc[:, s.dim:].astype(BF16)


def call(kernel, outs, args, flops, scratch=(), space=pltpu.VMEM):
    specs = [pl.BlockSpec(memory_space=space)] * len(args)
    if space == pltpu.HBM:
        args = [pltpu.with_memory_space_constraint(a, space) for a in args]
    return pl.pallas_call(
        kernel,
        out_shape=outs,
        in_specs=specs,
        out_specs=jax.tree.map(lambda _: pl.BlockSpec(memory_space=pltpu.VMEM), outs),
        scratch_shapes=scratch,
        compiler_params=pltpu.CompilerParams(vmem_limit_bytes=VMEM_GRANT),
        cost_estimate=pl.CostEstimate(flops=flops, bytes_accessed=1 << 20, transcendentals=0),
    )(*args)


def on_device(query_a, key_a, value_a, grad_out_a, query_b, key_b, value_b, slab_owner):
    devices = lax.axis_size("context")
    tok, width = query_a.shape
    s = Shape(tok, width, key_a.shape[1], devices)
    dim, group = s.dim, s.group

    def swapped(x, bits):
        return lax.ppermute(x, "context", [(i, i ^ bits) for i in range(devices)])

    def sds(shape, dtype):
        return jax.ShapeDtypeStruct(shape, dtype)

    unit = 2 * 4 * group * s.keys * dim
    pair, stack = sds((tok, 2 * dim), BF16), sds((4 * group, dim), BF16)
    kv_a = call(
        partial(fetch_kernel, s), pair, [key_a, value_a], unit,
        space=pltpu.HBM, scratch=[pltpu.SemaphoreType.DMA((2,))],
    )
    near = [swapped(kv_a, 2 * k) for k in range(1, s.chunks)]
    kv_b, rows, gap = call(
        partial(fetch_rest_kernel, s),
        [pair, sds((tok, 3 * width), BF16), sds((2 * s.chunks, group), jnp.int32)],
        [slab_owner, key_b, value_b, query_a, grad_out_a, query_b], unit,
        space=pltpu.HBM, scratch=[pltpu.SMEM((devices,), jnp.int32), pltpu.SemaphoreType.DMA((6,))],
    )
    kv_a = [kv_a] + near
    rows_p = swapped(rows, 1)
    kv_b = [kv_b] + [swapped(kv_b, 2 * k) for k in range(1, s.chunks)]
    q_a, g_a, q_b = call(partial(stack_kernel, s), [stack] * 3, [rows, rows_p], unit)
    mine = call(partial(stats_kernel, s), sds((8, 4 * group), F32), [gap, q_a, g_a, *kv_a], 8 * unit)
    theirs = swapped(mine, 1)
    kinds = [F32] + [BF16] * (s.chunks - 1)
    back = call(
        partial(back_kernel, s),
        [sds((tok, 2 * dim), kind) for kind in kinds] + [sds((dim, 2 * group), F32)] * 2,
        [gap, q_a, g_a, mine, theirs, *kv_a], 20 * unit,
        scratch=[pltpu.VMEM((2 * s.keys, 4 * group), BF16)] * 2,
    )
    terms, (dq_own, dq_other) = back[:s.chunks], back[s.chunks:]
    terms = [terms[0]] + [swapped(terms[k], 2 * k) for k in range(1, s.chunks)]
    send = call(
        partial(other_kernel, s), sds((2 * dim + 8, 2 * group), F32),
        [gap, q_b, dq_other, *kv_b], 5 * unit,
    )
    got = swapped(send, 1)
    part = call(partial(own_kernel, s), sds((dim + 8, 2 * group), F32), [gap, q_b, send, *kv_b], 5 * unit)
    out_b, grad_query_a = call(partial(rows_kernel, s), [sds((tok, width), BF16)] * 2, [part, dq_own, got], unit)
    grad_key_a, grad_value_a = call(partial(sum_kernel, s), [sds((tok, dim), BF16)] * 2, terms, unit)
    return (out_b, grad_query_a, grad_key_a, grad_value_a)


def solution(mesh):
    rows = P(("dp", "context"), "tensor")

    return jax.shard_map(
        on_device,
        mesh=mesh,
        in_specs=(rows,) * 7 + (P(),),
        out_specs=(rows,) * 4,
        check_vma=False,
    )
```

```python
from functools import partial
import math

import jax
import jax.numpy as jnp
from jax import lax
from jax.experimental import pallas as pl
from jax.experimental.pallas import tpu as pltpu
from jax.sharding import PartitionSpec as P


LOW = -1e30
FLOOR = -1e20
TINY = 1e-30
F32 = jnp.float32
BF16 = jnp.bfloat16
LOG2E = math.log2(math.e)
VMEM_GRANT = 24 << 20


def dot(a, b, dims):
    return lax.dot_general(a, b, (dims, ((), ())), preferred_element_type=F32)


class Shape:
    def __init__(self, tok, width, dim, devices):
        self.tok, self.width, self.dim, self.devices = tok, width, dim, devices
        self.half = tok // 2
        self.heads = width // dim
        self.chunks = devices // 2
        self.group = self.heads * self.half
        self.keys = self.chunks * self.half
        self.scale = dim ** (-0.5)
        self.exp_scale = self.scale * LOG2E


def stacked(s, own_ref, other_ref):
    parts = []
    for h in range(2):
        for ref in (own_ref, other_ref):
            for g in range(s.heads):
                parts.append(ref[h * s.half:(h + 1) * s.half, g * s.dim:(g + 1) * s.dim])
    return jnp.concatenate(parts, axis=0)


def halves(s, chunk_refs, part):
    cols = slice(part * s.dim, (part + 1) * s.dim)
    low = jnp.concatenate([r[:s.half, cols] for r in chunk_refs], axis=0)
    high = jnp.concatenate([r[s.half:, cols] for r in chunk_refs], axis=0)
    return low, high


def relative(s):
    key = lax.broadcasted_iota(jnp.int32, (s.half, s.group), 0)
    row = lax.broadcasted_iota(jnp.int32, (s.half, s.group), 1) % s.half
    return key - row


def masked(s, scores, rel, gap_ref, d, high, names=None):
    parts = []
    for i, k in enumerate(range(s.chunks) if names is None else names):
        gap = gap_ref[d * s.chunks + k:d * s.chunks + k + 1, :]
        block = scores[i * s.half:(i + 1) * s.half, :]
        parts.append(jnp.where(rel <= (-gap if high else gap), block, LOW))
    return jnp.concatenate(parts, axis=0)


def fetch_kernel(s, keys, values, out, sems):
    left = pltpu.make_async_copy(keys, out.at[:, pl.ds(0, s.dim)], sems.at[0])
    right = pltpu.make_async_copy(values, out.at[:, pl.ds(s.dim, s.dim)], sems.at[1])
    left.start()
    right.start()
    left.wait()
    right.wait()


def fetch_rest_kernel(s, owner, kb, vb, qa, ga, qb, kv_b, rows, gap, slabs, sems):
    moves = [(owner, slabs), (kb, kv_b.at[:, pl.ds(0, s.dim)]), (vb, kv_b.at[:, pl.ds(s.dim, s.dim)])]
    moves += [(x, rows.at[:, pl.ds(i * s.width, s.width)]) for i, x in enumerate((qa, ga, qb))]
    copies = [pltpu.make_async_copy(a, b, sems.at[i]) for i, (a, b) in enumerate(moves)]
    for c in copies:
        c.start()
    copies[0].wait()
    me = lax.axis_index("context")
    for d in range(2):
        for k in range(s.chunks):
            ahead = (slabs[me ^ d] - slabs[me ^ (2 * k)]) * s.half
            gap[d * s.chunks + k:d * s.chunks + k + 1, :] = jnp.full((1, s.group), ahead, jnp.int32)
    for c in copies[1:]:
        c.wait()


def stack_kernel(s, own_ref, other_ref, *out_refs):
    for i, ref in enumerate(out_refs):
        cols = slice(i * s.width, (i + 1) * s.width)
        ref[...] = stacked(s, own_ref[:, cols], other_ref[:, cols])


def stats_kernel(s, gap_ref, q_ref, g_ref, *refs):
    chunks, out_ref = refs[:-1], refs[-1]
    q, g = q_ref[...], g_ref[...]
    k_low, k_high = halves(s, chunks, 0)
    v_low, v_high = halves(s, chunks, 1)
    rel = relative(s)
    for h in range(2):
        for d in range(2):
            at = (2 * h + d) * s.group
            qt, gt = q[at:at + s.group], g[at:at + s.group]
            raw = dot(k_low, qt, ((1,), (1,)))
            pg = dot(v_low, gt, ((1,), (1,)))
            if h == 0:
                raw = masked(s, raw, rel, gap_ref, d, False)
                blocks = [(raw, pg)]
            else:
                more = masked(s, dot(k_high, qt, ((1,), (1,))), rel, gap_ref, d, True)
                blocks = [(raw, pg), (more, dot(v_high, gt, ((1,), (1,))))]
            top = jnp.full((1, s.group), FLOOR, F32)
            for raw, pg in blocks:
                top = jnp.maximum(top, jnp.max(raw, axis=0, keepdims=True))
            total = jnp.zeros((1, s.group), F32)
            dsum = jnp.zeros((1, s.group), F32)
            for raw, pg in blocks:
                p = jnp.exp2((raw - top) * s.exp_scale)
                total = total + jnp.sum(p, axis=0, keepdims=True)
                dsum = dsum + jnp.sum(p * pg, axis=0, keepdims=True)
            out_ref[0:1, at:at + s.group] = top
            out_ref[1:2, at:at + s.group] = total
            out_ref[2:3, at:at + s.group] = dsum
    out_ref[3:8, :] = jnp.zeros((5, 4 * s.group), F32)


def back_terms(s, names, gap_ref, q_ref, g_ref, mine_ref, theirs_ref, chunks, out_refs, prob_ref, grad_ref):
    k_low, k_high = halves(s, chunks, 0)
    v_low, v_high = halves(s, chunks, 1)
    rel = relative(s)
    group, keys = s.group, k_low.shape[0]
    for h in range(2):
        for d in range(2):
            at, across = (2 * h + d) * group, (2 * h + 1 - d) * group
            m1, l1, d1 = (mine_ref[i:i + 1, at:at + group] for i in range(3))
            m2, l2, d2 = (theirs_ref[i:i + 1, across:across + group] for i in range(3))
            top = jnp.maximum(m1, m2)
            w1, w2 = jnp.exp2((m1 - top) * s.exp_scale), jnp.exp2((m2 - top) * s.exp_scale)
            total = l1 * w1 + l2 * w2
            delta = (d1 * w1 + d2 * w2) / total
            shift = top * s.exp_scale + jnp.log2(total)
            qt, gt = q_ref[at:at + group], g_ref[at:at + group]
            for b in range(h + 1):
                kk, vv = (k_low, v_low) if b == 0 else (k_high, v_high)
                raw = dot(kk, qt, ((1,), (1,)))
                pg = dot(vv, gt, ((1,), (1,)))
                if b == h:
                    raw = masked(s, raw, rel, gap_ref, d, h == 1, names)
                p = jnp.exp2(raw * s.exp_scale - shift)
                prob_ref[b * keys:(b + 1) * keys, at:at + group] = p.astype(BF16)
                grad_ref[b * keys:(b + 1) * keys, at:at + group] = (p * (pg - delta)).astype(BF16)
    mid = 2 * group
    dk_low = dot(grad_ref[:keys, :], q_ref[...], ((1,), (0,))) * s.scale
    dv_low = dot(prob_ref[:keys, :], g_ref[...], ((1,), (0,)))
    dk_high = dot(grad_ref[keys:, mid:], q_ref[mid:], ((1,), (0,))) * s.scale
    dv_high = dot(prob_ref[keys:, mid:], g_ref[mid:], ((1,), (0,)))
    for k, ref in enumerate(out_refs):
        at = slice(k * s.half, (k + 1) * s.half)
        for h, (dk, dv) in enumerate(((dk_low, dv_low), (dk_high, dv_high))):
            rows = slice(h * s.half, (h + 1) * s.half)
            ref[rows, :s.dim] = dk[at].astype(ref.dtype)
            ref[rows, s.dim:] = dv[at].astype(ref.dtype)


def far_kernel(s, gap_ref, q_ref, g_ref, mine_ref, theirs_ref, *refs):
    n = s.chunks - s.chunks // 2
    names = range(s.chunks // 2, s.chunks)
    back_terms(
        s, names, gap_ref, q_ref, g_ref, mine_ref, theirs_ref, refs[:n], refs[n:2 * n], refs[-1], refs[-2]
    )


def near_kernel(s, gap_ref, q_ref, g_ref, mine_ref, theirs_ref, far_grad_ref, *refs):
    n, count = s.chunks // 2, s.chunks
    chunks, outs = refs[:count], refs[count:count + n]
    dq_own_ref, dq_other_ref, prob_ref, grad_ref = refs[count + n:]
    back_terms(
        s, range(n), gap_ref, q_ref, g_ref, mine_ref, theirs_ref, chunks[:n], outs, prob_ref, grad_ref
    )
    group, mid = s.group, 2 * s.group
    low_rows = high_rows = 0.0
    for part, ref in ((chunks[:n], grad_ref), (chunks[n:], far_grad_ref)):
        k_low, k_high = halves(s, part, 0)
        keys = k_low.shape[0]
        low_rows = low_rows + dot(k_low, ref[:keys, :mid], ((0,), (0,)))
        high_rows = high_rows + dot(k_low, ref[:keys, mid:], ((0,), (0,)))
        high_rows = high_rows + dot(k_high, ref[keys:, mid:], ((0,), (0,)))
    for d, ref in enumerate((dq_own_ref, dq_other_ref)):
        ref[:, :group] = low_rows[:, d * group:(d + 1) * group]
        ref[:, group:] = high_rows[:, d * group:(d + 1) * group]


def forward_rows(s, d, gap_ref, q_ref, chunks, out_ref):
    k_low, k_high = halves(s, chunks, 0)
    v_low, v_high = halves(s, chunks, 1)
    rel = relative(s)
    for h in range(2):
        at = (2 * h + d) * s.group
        qt = q_ref[at:at + s.group]
        raw = dot(k_low, qt, ((1,), (1,)))
        if h == 0:
            blocks = [(masked(s, raw, rel, gap_ref, d, False), v_low)]
        else:
            more = dot(k_high, qt, ((1,), (1,)))
            blocks = [(raw, v_low), (masked(s, more, rel, gap_ref, d, True), v_high)]
        top = jnp.full((1, s.group), FLOOR, F32)
        for raw, vv in blocks:
            top = jnp.maximum(top, jnp.max(raw, axis=0, keepdims=True))
        total = jnp.zeros((1, s.group), F32)
        acc = jnp.zeros((s.dim, s.group), F32)
        for raw, vv in blocks:
            p = jnp.exp2((raw - top) * s.exp_scale)
            total = total + jnp.sum(p, axis=0, keepdims=True)
            acc = acc + dot(vv, p.astype(BF16), ((0,), (0,)))
        cols = slice(h * s.group, (h + 1) * s.group)
        total = jnp.maximum(total, TINY)
        out_ref[:s.dim, cols] = (acc / total).astype(out_ref.dtype)
        log_total = top * s.exp_scale + jnp.log2(total)
        if out_ref.dtype == F32:
            out_ref[s.dim:, cols] = jnp.broadcast_to(log_total, (8, s.group))
        else:
            parts, rest = [], log_total
            for _ in range(3):
                parts.append(rest.astype(BF16).astype(F32))
                rest = rest - parts[-1]
            rows = jnp.concatenate([*parts, jnp.zeros((13, s.group), F32)], axis=0)
            out_ref[s.dim:s.dim + 16, cols] = rows.astype(BF16)


def other_kernel(s, gap_ref, q_ref, dq_ref, *refs):
    chunks, out_ref = refs[:-1], refs[-1]
    forward_rows(s, 1, gap_ref, q_ref, chunks, out_ref)
    out_ref[s.dim + 16:, :] = dq_ref[...].astype(BF16)


def own_kernel(s, gap_ref, q_ref, after, *refs):
    forward_rows(s, 0, gap_ref, q_ref, refs[:-1], refs[-1])


def rows_from(s, wide, out_ref):
    for h in range(2):
        for g in range(s.heads):
            at = h * s.group + g * s.half
            block = wide[:, at:at + s.half]
            out_ref[h * s.half:(h + 1) * s.half, g * s.dim:(g + 1) * s.dim] = block.T.astype(BF16)


def rows_kernel(s, own_ref, dq_ref, got_ref, out_ref, query_ref):
    d = s.dim
    rows_from(s, (dq_ref[...] + got_ref[d + 16:, :].astype(F32)) * s.scale, query_ref)
    logs = got_ref[d:d + 16, :].astype(F32)
    l1, l2 = own_ref[d:d + 1, :], logs[0:1] + logs[1:2] + logs[2:3]
    top = jnp.maximum(l1, l2)
    w1, w2 = jnp.exp2(l1 - top), jnp.exp2(l2 - top)
    total = w1 + w2
    rows_from(s, own_ref[:d, :] * (w1 / total) + got_ref[:d, :].astype(F32) * (w2 / total), out_ref)


def sum_kernel(s, *refs):
    terms, (key_ref, value_ref) = refs[:-2], refs[-2:]
    acc = terms[0][...]
    for t in terms[1:]:
        acc = acc + t[...].astype(F32)
    key_ref[...] = acc[:, :s.dim].astype(BF16)
    value_ref[...] = acc[:, s.dim:].astype(BF16)


def call(kernel, outs, args, flops, scratch=(), space=pltpu.VMEM):
    specs = [pl.BlockSpec(memory_space=space)] * len(args)
    if space == pltpu.HBM:
        args = [pltpu.with_memory_space_constraint(a, space) for a in args]
    return pl.pallas_call(
        kernel,
        out_shape=outs,
        in_specs=specs,
        out_specs=jax.tree.map(lambda _: pl.BlockSpec(memory_space=pltpu.VMEM), outs),
        scratch_shapes=scratch,
        compiler_params=pltpu.CompilerParams(vmem_limit_bytes=VMEM_GRANT),
        cost_estimate=pl.CostEstimate(flops=flops, bytes_accessed=1 << 20, transcendentals=0),
    )(*args)


def on_device(query_a, key_a, value_a, grad_out_a, query_b, key_b, value_b, slab_owner):
    devices = lax.axis_size("context")
    tok, width = query_a.shape
    s = Shape(tok, width, key_a.shape[1], devices)
    dim, group = s.dim, s.group

    def swapped(x, bits):
        return lax.ppermute(x, "context", [(i, i ^ bits) for i in range(devices)])

    def sds(shape, dtype):
        return jax.ShapeDtypeStruct(shape, dtype)

    unit = 2 * 4 * group * s.keys * dim
    pair, stack = sds((tok, 2 * dim), BF16), sds((4 * group, dim), BF16)
    kv_a = call(
        partial(fetch_kernel, s), pair, [key_a, value_a], unit,
        space=pltpu.HBM, scratch=[pltpu.SemaphoreType.DMA((2,))],
    )
    near = [swapped(kv_a, 2 * k) for k in range(1, s.chunks)]
    kv_b, rows, gap = call(
        partial(fetch_rest_kernel, s),
        [pair, sds((tok, 3 * width), BF16), sds((2 * s.chunks, group), jnp.int32)],
        [slab_owner, key_b, value_b, query_a, grad_out_a, query_b], unit,
        space=pltpu.HBM, scratch=[pltpu.SMEM((devices,), jnp.int32), pltpu.SemaphoreType.DMA((6,))],
    )
    kv_a = [kv_a] + near
    rows_p = swapped(rows, 1)
    kv_b = [kv_b] + [swapped(kv_b, 2 * k) for k in range(1, s.chunks)]
    q_a, g_a, q_b = call(partial(stack_kernel, s), [stack] * 3, [rows, rows_p], unit)
    mine = call(partial(stats_kernel, s), sds((8, 4 * group), F32), [gap, q_a, g_a, *kv_a], 8 * unit)
    theirs = swapped(mine, 1)
    near = s.chunks // 2
    kinds = [F32] + [BF16] * (s.chunks - 1)
    terms = [sds((tok, 2 * dim), kind) for kind in kinds]
    score = (2 * near * s.half, 4 * group)
    *far_terms, far_grad = call(
        partial(far_kernel, s), [*terms[near:], sds(score, BF16)],
        [gap, q_a, g_a, mine, theirs, *kv_a[near:]], 10 * unit, scratch=[pltpu.VMEM(score, BF16)],
    )
    *near_terms, dq_own, dq_other = call(
        partial(near_kernel, s), [*terms[:near], *[sds((dim, 2 * group), F32)] * 2],
        [gap, q_a, g_a, mine, theirs, far_grad, *kv_a], 10 * unit, scratch=[pltpu.VMEM(score, BF16)] * 2,
    )
    terms = [*near_terms, *far_terms]
    terms = [terms[0]] + [swapped(terms[k], 2 * k) for k in range(1, s.chunks)]
    send = call(
        partial(other_kernel, s), sds((2 * dim + 16, 2 * group), BF16),
        [gap, q_b, dq_other, *kv_b], 5 * unit,
    )
    got = swapped(send, 1)
    part = call(partial(own_kernel, s), sds((dim + 8, 2 * group), F32), [gap, q_b, send, *kv_b], 5 * unit)
    out_b, grad_query_a = call(partial(rows_kernel, s), [sds((tok, width), BF16)] * 2, [part, dq_own, got], unit)
    grad_key_a, grad_value_a = call(partial(sum_kernel, s), [sds((tok, dim), BF16)] * 2, terms, unit)
    return (out_b, grad_query_a, grad_key_a, grad_value_a)


def solution(mesh):
    rows = P(("dp", "context"), "tensor")

    return jax.shard_map(
        on_device,
        mesh=mesh,
        in_specs=(rows,) * 7 + (P(),),
        out_specs=(rows,) * 4,
        check_vma=False,
    )
```
